128 devices in a mesh: pairs: 4 (over x, y), ctx: 32 (over z, core).
Axes of the slice: x: 2, y: 2, z: 16, core: 2. Of those that a mesh axis runs over, the one named last changes fastest.
The devices are a block of a 8x8x16 slice.
Arguments:
- prompt_keys: bfloat16 [4096, 512], P(('pairs', 'ctx')), parts along dimension 0, may hold values from -4 to 4
- prompt_values: bfloat16 [4096, 512], P(('pairs', 'ctx')), parts along dimension 0, may hold values from -6 to 6
- queries: bfloat16 [8, 1536, 4096], P('pairs', 'ctx'), parts along dimension 0, may hold values from -100 to 100
- resp_keys: bfloat16 [8, 1536, 512], P('pairs', 'ctx'), parts along dimension 0, may hold values from -6 to 6
- resp_values: bfloat16 [8, 1536, 512], P('pairs', 'ctx'), parts along dimension 0, may hold values from -6 to 6
- cotangent: bfloat16 [8, 1536, 4096], P('pairs', 'ctx'), parts along dimension 0, may hold values from -48 to 48
- lengths: int32 [8], P('pairs'), parts along dimension 0, may hold values from 384 to 1536, as said below
Outputs:
- grad_queries: float32 [8, 1536, 4096], P('pairs', 'ctx'), parts along dimension 0
- grad_resp_keys: float32 [8, 1536, 512], P('pairs', 'ctx'), parts along dimension 0
- grad_resp_values: float32 [8, 1536, 512], P('pairs', 'ctx'), parts along dimension 0
- grad_prompt_keys: float32 [4096, 512], P(('pairs', 'ctx')), parts along dimension 0
- grad_prompt_values: float32 [4096, 512], P(('pairs', 'ctx')), parts along dimension 0
The draws below stay inside these ranges and needn't reach their ends.
There are 4 independent parts, one for each index of `pairs`. The reference program is written for one: setup_inputs(seed, part) draws one part's arguments, and reference() takes and returns one part's arrays. A program takes and returns all parts, laid end to end along the dimension named above; each array names one. Nothing has to cross between parts.
Inputs may be any that keep to these rules, and one draw needn't show every extreme that they name: `lengths`: in every pair one of the two responses has all 1536 rows live.
All inputs are finite; a program needn't handle non-finite values.
Results may differ from the reference program's by a relative error of at most 0.005.
Values may be sent and summed in bfloat16 or wider, within the bound.
No kernel may reach another device: no remote copies, remote signals or barrier semaphores. Data moves between devices by JAX's collectives and lax.ppermute only.
A program may use at most 128 MiB of HBM per device.

```python
import math
import jax
import jax.numpy as jnp
from jax import lax

HEADS = 32
KV_HEADS = 4
HEAD_DIM = 128
RESP = 1536
PROMPT = 1024


def prompt_draw(key):
    return jax.random.truncated_normal(jax.random.fold_in(key, 11), -4.0, 4.0, (PROMPT, KV_HEADS * HEAD_DIM), jnp.float32)


def draw_prompt_keys(key, part):
    return prompt_draw(key).astype(jnp.bfloat16)


def draw_queries(key, part):
    normal_part = jax.random.normal(jax.random.fold_in(key, 23), (2, RESP, HEADS * HEAD_DIM), jnp.float32)
    result = jnp.clip(normal_part, -6.0, 6.0)
    return result.astype(jnp.bfloat16)


def draw_lengths(key, part):
    shorter = jax.random.randint(jax.random.fold_in(key, 41), (), RESP // 4, RESP + 1).astype(jnp.int32)
    longer = jnp.full((), RESP, jnp.int32)
    which = jax.random.randint(jax.random.fold_in(key, 43), (), 0, 2)
    return jnp.where(which == 0, jnp.stack([longer, shorter]), jnp.stack([shorter, longer])).astype(jnp.int32)


def level_of(key, dims, pieces, least, high):
    level, own = 1.0, jax.random.fold_in(key, 6)
    for position, shards_of in pieces:
        draws = jnp.exp(jax.random.uniform(jax.random.fold_in(own, position), (shards_of,), jnp.float32, least / len(pieces), high / len(pieces)))
        level = level * jnp.repeat(draws, dims[position] // shards_of).reshape([-1 if axis == position else 1 for axis in range(len(dims))])
    return level


def bell_draw(own_key, shape, deviation, limit, cuts=(), kind=jnp.bfloat16):
    values = jax.random.normal(own_key, shape, jnp.float32) * deviation
    if len(cuts) > 0:
        values = level_of(own_key, shape, cuts, -0.22, 0.18) * values
    return jnp.clip(values, min=-limit, max=limit).astype(kind)


def setup_inputs(seed: int = 0, part: int = 0) -> dict:
    arg_keys = jax.random.split(jax.random.key(seed), 8)
    own_keys = jax.random.split(jax.random.fold_in(arg_keys[7], part), 8)
    return {
        "prompt_keys": draw_prompt_keys(jax.random.fold_in(jax.random.fold_in(arg_keys[7], part), 71), part),
        "prompt_values": bell_draw(own_keys[1], (PROMPT, KV_HEADS * HEAD_DIM), 1.0, 6.0, ((0, 32),)),
        "queries": draw_queries(jax.random.fold_in(jax.random.fold_in(arg_keys[7], part), 71), part),
        "resp_keys": bell_draw(own_keys[3], (2, RESP, KV_HEADS * HEAD_DIM), 1.0, 6.0, ((1, 32),)),
        "resp_values": bell_draw(own_keys[4], (2, RESP, KV_HEADS * HEAD_DIM), 1.0, 6.0, ((1, 32),)),
        "cotangent": jnp.clip(jax.random.uniform(own_keys[5], (2, RESP, HEADS * HEAD_DIM), jnp.float32, -48.0, 48.0) * level_of(own_keys[5], (2, RESP, HEADS * HEAD_DIM), ((1, 32),), -0.4, 0.0), -48.0, 48.0).astype(jnp.bfloat16),
        "lengths": draw_lengths(jax.random.fold_in(jax.random.fold_in(arg_keys[7], part), 71), part),
    }


def rounded(array):
    return lax.optimization_barrier(array.astype(jnp.bfloat16)).astype(jnp.float32)


def one_branch(query_rows, cotangent_rows, key_rows, value_rows, length):
    group_size = HEADS // KV_HEADS
    score_scale = HEAD_DIM ** -0.5
    total_keys = key_rows.shape[0]
    keys_all = key_rows.reshape(total_keys, KV_HEADS, HEAD_DIM).astype(jnp.float32)
    values_all = value_rows.reshape(total_keys, KV_HEADS, HEAD_DIM).astype(jnp.float32)
    key_positions = jnp.arange(total_keys, dtype=jnp.int32) - PROMPT
    height = math.gcd(RESP, 256)
    number = RESP // height
    query_blocks = query_rows.reshape(number, height, KV_HEADS, group_size, HEAD_DIM)
    cotangent_blocks = cotangent_rows.reshape(number, height, KV_HEADS, group_size, HEAD_DIM)

    def advance(carried, element):
        key_sum, value_sum = carried
        queries, upstream, block_index = element
        positions = block_index * height + jnp.arange(height, dtype=jnp.int32)
        live_rows = positions < length
        queries = queries.astype(jnp.float32)
        upstream = jnp.where(live_rows[:, None, None, None], upstream.astype(jnp.float32), 0.0)
        scores = jnp.einsum("qkgd,nkd->kgqn", queries, keys_all) * score_scale
        scores = jnp.where(key_positions[None, :] <= positions[:, None], scores, -jnp.inf)
        log_norm = jax.nn.logsumexp(scores, axis=-1)
        probs = jnp.exp(scores - log_norm[..., None])
        probs_low = rounded(probs)
        attended = jnp.einsum("kgqn,nkd->kgqd", probs_low, values_all)
        attended = rounded(jnp.where(live_rows[None, None, :, None], attended, 0.0))
        delta = jnp.einsum("qkgd,kgqd->kgq", upstream, attended)
        prob_grad = jnp.einsum("qkgd,nkd->kgqn", upstream, values_all)
        score_grad = rounded(probs * (prob_grad - delta[..., None]))
        query_grad = jnp.einsum("kgqn,nkd->qkgd", score_grad, keys_all) * score_scale
        key_sum = key_sum + jnp.einsum("kgqn,qkgd->nkd", score_grad, queries) * score_scale
        value_sum = value_sum + jnp.einsum("kgqn,qkgd->nkd", probs_low, upstream)
        return (key_sum, value_sum), query_grad.reshape(height, HEADS * HEAD_DIM)

    empty_sum = jnp.zeros((total_keys, KV_HEADS, HEAD_DIM), jnp.float32)
    indices = jnp.arange(number, dtype=jnp.int32)
    (key_sum, value_sum), query_grads = lax.scan(advance, (empty_sum, empty_sum), (query_blocks, cotangent_blocks, indices))
    width = KV_HEADS * HEAD_DIM
    return query_grads.reshape(RESP, HEADS * HEAD_DIM), key_sum.reshape(total_keys, width), value_sum.reshape(total_keys, width)


def reference(prompt_keys, prompt_values, queries, resp_keys, resp_values, cotangent, lengths):
    query_grads = []
    resp_key_grads = []
    resp_value_grads = []
    prompt_key_sum = jnp.zeros(prompt_keys.shape, jnp.float32)
    prompt_value_sum = jnp.zeros(prompt_values.shape, jnp.float32)
    for branch in range(2):
        key_rows = jnp.concatenate([prompt_keys, resp_keys[branch]], axis=0)
        value_rows = jnp.concatenate([prompt_values, resp_values[branch]], axis=0)
        grad_rows, key_grad, value_grad = one_branch(queries[branch], cotangent[branch], key_rows, value_rows, lengths[branch])
        query_grads.append(grad_rows)
        prompt_key_sum = prompt_key_sum + key_grad[:PROMPT]
        prompt_value_sum = prompt_value_sum + value_grad[:PROMPT]
        resp_key_grads.append(key_grad[PROMPT:])
        resp_value_grads.append(value_grad[PROMPT:])
    return (jnp.stack(query_grads), jnp.stack(resp_key_grads), jnp.stack(resp_value_grads), prompt_key_sum, prompt_value_sum)
```

```python
import functools
import math

import jax
import jax.numpy as jnp
from jax import lax
from jax.experimental import pallas as pl
from jax.experimental.pallas import tpu as pltpu
from jax.sharding import Mesh
from jax.sharding import PartitionSpec as P

HEADS = 32
KV_HEADS = 4
D = 128
GROUP = HEADS // KV_HEADS
OWN = KV_HEADS // 2
SCALE = D ** (-0.5)
TO_LOG2 = SCALE * math.log2(math.e)
LOW = -1e30
COLS = 256


f32 = jnp.float32
bf16 = jnp.bfloat16
VMEM = pl.BlockSpec(memory_space=pltpu.VMEM)
SMEM = pl.BlockSpec(memory_space=pltpu.SMEM)


def nt(a, b):
    return lax.dot_general(a, b, (((1,), (1,)), ((), ())), preferred_element_type=f32)


def nn(a, b):
    return lax.dot_general(a, b, (((1,), (0,)), ((), ())), preferred_element_type=f32)


def cost(flops, nbytes):
    return pl.CostEstimate(flops=int(flops), bytes_accessed=int(nbytes), transcendentals=0)


def pack_kernel(who, pk, pv, rk, rv, mine, send):
    core = who[1]
    prompt, rows = pk.shape[0], rk.shape[1]
    for dst, side in ((mine, core), (send, 1 - core)):
        for j in range(OWN):
            lanes = pl.ds(pl.multiple_of((side * OWN + j) * D, D), D)
            for k, (p_ref, r_ref) in enumerate(((pk, rk), (pv, rv))):
                out = pl.ds(k * D, D)
                dst[j, 0:prompt, out] = p_ref[:, lanes]
                for b in range(2):
                    at = prompt + b * rows
                    dst[j, at : at + rows, out] = r_ref[b, :, lanes]


def pack_kv(who, pk, pv, rk, rv):
    rows = pk.shape[0] + 2 * rk.shape[1]
    shape = jax.ShapeDtypeStruct((OWN, rows, 2 * D), bf16)
    return pl.pallas_call(
        pack_kernel,
        out_shape=(shape, shape),
        in_specs=[SMEM, VMEM, VMEM, VMEM, VMEM],
        out_specs=(VMEM, VMEM),
        name="pack_kv",
    )(who, pk, pv, rk, rv)


def parts_of(prompt, rows):
    return (
        (0, 0, prompt),
        (prompt, 2 * prompt, rows),
        (prompt + rows, 2 * prompt + 2 * rows, rows),
    )


def join_kernel(parts, who, mine, other, *outs):
    core = who[1]
    for src, side in ((mine, core), (other, 1 - core)):
        for j in range(OWN):
            for at, chip_at, n in parts:
                to = pl.ds(pl.multiple_of(chip_at + side * n, 16), n)
                outs[j][to, :] = src[j, at : at + n, :]


def join_kv(parts, who, mine, other):
    shape = jax.ShapeDtypeStruct((2 * mine.shape[1], 2 * D), bf16)
    return pl.pallas_call(
        functools.partial(join_kernel, parts),
        out_shape=(shape,) * OWN,
        in_specs=[SMEM, VMEM, VMEM],
        out_specs=(VMEM,) * OWN,
        name="join_kv",
    )(who, mine, other)


def prep_kernel(who, q_mine, q_other, c_mine, c_other, q_out, u_out):
    b = pl.program_id(1)
    place, core, live = who[0], who[1], who[2 + b]
    rows = q_mine.shape[1]
    for side, q_ref, c_ref in ((core, q_mine, c_mine), (1 - core, q_other, c_other)):
        first = place * (2 * rows) + side * rows
        alive = first + lax.broadcasted_iota(jnp.int32, (rows, D), 0) < live
        for g in range(GROUP):
            to = pl.ds(pl.multiple_of(g * 2 * rows + side * rows, 16), rows)
            q_out[0, to, :] = q_ref[0, :, g * D : (g + 1) * D]
            u = c_ref[0, :, g * D : (g + 1) * D].astype(f32)
            u_out[0, to, :] = jnp.where(alive, u, 0.0).astype(bf16)


def prep(who, q_all, q_other, c_all, c_other):
    rows = q_all.shape[1]
    wide = GROUP * D
    shape = jax.ShapeDtypeStruct((OWN * 2, 2 * rows * GROUP, D), bf16)
    whole = pl.BlockSpec((1, rows, wide), lambda h, b, who: (b, 0, who[1] * OWN + h))
    half = pl.BlockSpec((1, rows, wide), lambda h, b, who: (b, 0, h))
    out = pl.BlockSpec((1, 2 * rows * GROUP, D), lambda h, b, who: (h * 2 + b, 0, 0))
    return pl.pallas_call(
        prep_kernel,
        out_shape=(shape, shape),
        grid_spec=pltpu.PrefetchScalarGridSpec(
            num_scalar_prefetch=1,
            grid=(OWN, 2),
            in_specs=[whole, half, whole, half],
            out_specs=(out, out),
        ),
        cost_estimate=cost(1e6, 6e6),
        name="prep",
    )(who, q_all, q_other, c_all, c_other)


def load_keys(kv_refs, parts, ks, vs):
    h, b = pl.program_id(0), pl.program_id(1)
    prompt, rows = 2 * parts[0][2], 2 * parts[1][2]
    n = len(kv_refs)
    here = pl.ds(pl.multiple_of(prompt + b * rows, 16), rows)
    for i, pair in enumerate(kv_refs):
        top = jnp.where(h == 0, pair[0][0:prompt, :], pair[1][0:prompt, :])
        low = jnp.where(h == 0, pair[0][here, :], pair[1][here, :])
        ks[i * prompt : (i + 1) * prompt, :] = top[:, :D]
        vs[i * prompt : (i + 1) * prompt, :] = top[:, D:]
        at = n * prompt + i * rows
        ks[at : at + rows, :] = low[:, :D]
        vs[at : at + rows, :] = low[:, D:]


def masked_scores(who, n, parts, ks, q, at_rows, cols):
    prompt, rows = 2 * parts[0][2], 2 * parts[1][2]
    s = nt(ks[...], q) * TO_LOG2
    place = at_rows[0:1, cols]
    pieces = [s[: n * prompt]]
    r = lax.broadcasted_iota(jnp.int32, (rows, q.shape[0]), 0)
    for i in range(n):
        at = n * prompt + i * rows
        seen = r <= place - who[4 + i] * rows
        pieces.append(jnp.where(seen, s[at : at + rows], -jnp.inf))
    return jnp.concatenate(pieces, axis=0)


def by_eights(x):
    return x.reshape(x.shape[0] // 8, 8, x.shape[1])


def stats_kernel(n, parts, first, *refs):
    who = refs[0]
    kv = [refs[1 + 2 * i : 3 + 2 * i] for i in range(n)]
    q_ref, u_ref, at_rows = refs[1 + 2 * n : 4 + 2 * n]
    if first:
        out, ks, vs = refs[4 + 2 * n :]
    else:
        old, out, ks, vs = refs[4 + 2 * n :]
    load_keys(kv, parts, ks, vs)

    def tile(t, _):
        cols = pl.ds(pl.multiple_of(t * COLS, COLS), COLS)
        s = masked_scores(who, n, parts, ks, q_ref[0, cols, :], at_rows, cols)
        dp = nt(vs[...], u_ref[0, cols, :])
        peak = jnp.max(by_eights(s), axis=0)
        peak = jnp.maximum(peak, LOW if first else old[0, 0, :, cols])
        p = jnp.exp2(by_eights(s) - peak[None])
        total = jnp.sum(p, axis=0)
        dot = jnp.sum(p * by_eights(dp), axis=0)
        if not first:
            fade = jnp.exp2(old[0, 0, :, cols] - peak)
            total = total + old[0, 1, :, cols] * fade
            dot = dot + old[0, 2, :, cols] * fade
        out[0, 0, :, cols] = peak
        out[0, 1, :, cols] = total
        out[0, 2, :, cols] = dot
        return 0

    lax.fori_loop(0, q_ref.shape[1] // COLS, tile, 0)


def keep_whole(shape):
    return pl.BlockSpec(shape, lambda h, b, who: (0,) * len(shape))


def by_step(shape):
    return pl.BlockSpec((1, *shape), lambda h, b, who: (h * 2 + b,) + (0,) * len(shape))


def stats(who, blocks, places, parts, q, u, at_rows, old):
    n = len(blocks)
    chip_rows = blocks[0][0].shape[0]
    wide = q.shape[1]
    keys = n * 2 * (parts[0][2] + parts[1][2])
    shape = jax.ShapeDtypeStruct((OWN * 2, 3, 8, wide), f32)
    flat = [a for pair in blocks for a in pair]
    in_specs = [keep_whole((chip_rows, 2 * D))] * (2 * n)
    in_specs += [by_step((wide, D)), by_step((wide, D)), keep_whole((8, wide))]
    operands = [jnp.concatenate([who, jnp.stack(places)]), *flat, q, u, at_rows]
    if old is not None:
        in_specs.append(by_step((3, 8, wide)))
        operands.append(old)
    return pl.pallas_call(
        functools.partial(stats_kernel, n, parts, old is None),
        out_shape=shape,
        grid_spec=pltpu.PrefetchScalarGridSpec(
            num_scalar_prefetch=1,
            grid=(OWN, 2),
            in_specs=in_specs,
            out_specs=by_step((3, 8, wide)),
            scratch_shapes=[pltpu.VMEM((keys, D), bf16), pltpu.VMEM((keys, D), bf16)],
        ),
        cost_estimate=cost(4 * 12 * keys * wide * D, 3e6),
        name=f"stats_{n}",
    )(*operands)


def grads_kernel(n, parts, first, *refs):
    who = refs[0]
    kv = [refs[1 + 2 * i : 3 + 2 * i] for i in range(n)]
    q_ref, u_ref, at_rows, st = refs[1 + 2 * n : 5 + 2 * n]
    refs = refs[5 + 2 * n :]
    if not first:
        dq_in, refs = refs[0], refs[1:]
    terms = [refs[2 * i : 2 * i + 2] for i in range(n)]
    dq, ks, vs, kt, dk, dv = refs[2 * n :]
    h, b = pl.program_id(0), pl.program_id(1)
    load_keys(kv, parts, ks, vs)
    kt[...] = ks[...].T
    dk[...] = jnp.zeros_like(dk)
    dv[...] = jnp.zeros_like(dv)

    def tile(t, _):
        cols = pl.ds(pl.multiple_of(t * COLS, COLS), COLS)
        q, u = q_ref[0, cols, :], u_ref[0, cols, :]
        peaks = st[0, 0, :, cols]
        peak = jnp.max(peaks, axis=0, keepdims=True)
        fade = jnp.exp2(peaks - peak)
        total = jnp.sum(st[0, 1, :, cols] * fade, axis=0, keepdims=True)
        part = 1.0 / total
        delta = jnp.sum(st[0, 2, :, cols] * fade, axis=0, keepdims=True) * part
        s = masked_scores(who, n, parts, ks, q, at_rows, cols)
        p = jnp.exp2(s - peak) * part
        dp = nt(vs[...], u)
        ds = (p * (dp - delta)).astype(bf16)
        dv[...] += nn(p.astype(bf16), u)
        dk[...] += nn(ds, q)
        more = nn(kt[...], ds)
        dq[0, :, cols] = more if first else dq_in[0, :, cols] + more
        return 0

    lax.fori_loop(0, q_ref.shape[1] // COLS, tile, 0)
    prompt, rows = 2 * parts[0][2], 2 * parts[1][2]
    here = pl.ds(pl.multiple_of(prompt + b * rows, 16), rows)
    for i in range(n):
        a, low = i * prompt, n * prompt + i * rows
        for j in range(OWN):

            @pl.when(h == j)
            def _(i=i, j=j, a=a, low=low):
                out = terms[i][j]
                for lane, ref, by in ((0, dk, SCALE), (D, dv, 1.0)):
                    lanes = pl.ds(lane, D)
                    top = ref[a : a + prompt, :] * by

                    @pl.when(b == 0)
                    def _():
                        out[0:prompt, lanes] = top

                    @pl.when(b != 0)
                    def _():
                        out[0:prompt, lanes] += top

                    out[here, lanes] = ref[low : low + rows, :] * by


def grads(who, blocks, places, parts, q, u, at_rows, st, dq):
    n = len(blocks)
    chip_rows = blocks[0][0].shape[0]
    wide = q.shape[1]
    keys = n * 2 * (parts[0][2] + parts[1][2])
    flat = [a for pair in blocks for a in pair]
    in_specs = [keep_whole((chip_rows, 2 * D))] * (2 * n)
    in_specs += [by_step((wide, D)), by_step((wide, D)), keep_whole((8, wide)), by_step((3, 8, wide))]
    operands = [jnp.concatenate([who, jnp.stack(places)]), *flat, q, u, at_rows, st]
    aliases = {}
    if dq is not None:
        in_specs.append(by_step((D, wide)))
        aliases = {len(operands): 2 * n}
        operands.append(dq)
    out = pl.pallas_call(
        functools.partial(grads_kernel, n, parts, dq is None),
        out_shape=(
            *[jax.ShapeDtypeStruct((chip_rows, 2 * D), f32)] * (2 * n),
            jax.ShapeDtypeStruct((OWN * 2, D, wide), f32),
        ),
        grid_spec=pltpu.PrefetchScalarGridSpec(
            num_scalar_prefetch=1,
            grid=(OWN, 2),
            in_specs=in_specs,
            out_specs=(*[keep_whole((chip_rows, 2 * D))] * (2 * n), by_step((D, wide))),
            scratch_shapes=[
                pltpu.VMEM((keys, D), bf16),
                pltpu.VMEM((keys, D), bf16),
                pltpu.VMEM((D, keys), bf16),
                pltpu.VMEM((keys, D), f32),
                pltpu.VMEM((keys, D), f32),
            ],
        ),
        input_output_aliases=aliases,
        cost_estimate=cost(4 * 20 * keys * wide * D, 6e6),
        name=f"grads_{n}",
    )(*operands)
    return [out[2 * i : 2 * i + 2] for i in range(n)], out[-1]


def finish_kernel(who, dq, own, other, turned):
    core = who[1]
    rows = own.shape[1]
    turned[...] = dq[0].T * SCALE
    for out, side in ((own, core), (other, 1 - core)):
        for g in range(GROUP):
            at = pl.ds(pl.multiple_of(g * 2 * rows + side * rows, 16), rows)
            out[0, :, g * D : (g + 1) * D] = turned[at, :]


def finish(who, dq, rows):
    wide = dq.shape[2]
    shape = jax.ShapeDtypeStruct((2, rows, OWN * GROUP * D), f32)
    out = pl.BlockSpec((1, rows, GROUP * D), lambda h, b, who: (b, 0, h))
    return pl.pallas_call(
        finish_kernel,
        out_shape=(shape, shape),
        grid_spec=pltpu.PrefetchScalarGridSpec(
            num_scalar_prefetch=1,
            grid=(OWN, 2),
            in_specs=[by_step((D, wide))],
            out_specs=(out, out),
            scratch_shapes=[pltpu.VMEM((wide, D), f32)],
        ),
        cost_estimate=cost(1e6, 4e6),
        name="finish",
    )(who, dq)


def split_kernel(parts, who, *refs):
    ins, (mine, send) = refs[:-2], refs[-2:]
    core = who[1]
    for dst, side in ((mine, core), (send, 1 - core)):
        for j in range(OWN):
            for at, chip_at, n in parts:
                src = pl.ds(pl.multiple_of(chip_at + side * n, 16), n)
                total = ins[j][src, :]
                for more in ins[OWN + j :: OWN]:
                    total = total + more[src, :].astype(f32)
                dst[j, at : at + n, :] = total


def split_rows(parts, who, own, arrived):
    rows = own[0].shape[0] // 2
    shape = jax.ShapeDtypeStruct((OWN, rows, 2 * D), f32)
    flat = [*own] + [a for pair in arrived for a in pair]
    return pl.pallas_call(
        functools.partial(split_kernel, parts),
        out_shape=(shape, shape),
        in_specs=[SMEM] + [VMEM] * len(flat),
        out_specs=(VMEM, VMEM),
        name="split_rows",
    )(who, *flat)


def emit_kernel(parts, who, mine, other, rk, rv, pk, pv):
    core = who[1]
    for src, side in ((mine, core), (other, 1 - core)):
        for j in range(OWN):
            lanes = pl.ds(pl.multiple_of((side * OWN + j) * D, D), D)
            for k, (p_ref, r_ref) in enumerate(((pk, rk), (pv, rv))):
                at, _, n = parts[0]
                p_ref[:, lanes] = src[j, at : at + n, k * D : (k + 1) * D]
                for b in range(2):
                    at, _, n = parts[1 + b]
                    r_ref[b, :, lanes] = src[j, at : at + n, k * D : (k + 1) * D]


def emit(parts, who, mine, other):
    prompt = jax.ShapeDtypeStruct((parts[0][2], KV_HEADS * D), f32)
    resp = jax.ShapeDtypeStruct((2, parts[1][2], KV_HEADS * D), f32)
    return pl.pallas_call(
        functools.partial(emit_kernel, parts),
        out_shape=(resp, resp, prompt, prompt),
        in_specs=[SMEM, VMEM, VMEM],
        out_specs=(VMEM,) * 4,
        name="emit",
    )(who, mine, other)


def local(prompt_keys, prompt_values, queries, resp_keys, resp_values, cotangent, lengths):
    ring = lax.axis_size("z")
    z, core = lax.axis_index("z"), lax.axis_index("core")
    rows = queries.shape[1]
    parts = parts_of(prompt_keys.shape[0], rows)
    who = jnp.stack([z, core, lengths[0], lengths[1]]).astype(jnp.int32)
    ups = [(i, (i + 1) % ring) for i in range(ring)]
    downs = [(i, (i - 1) % ring) for i in range(ring)]

    def swap(x):
        return lax.ppermute(x, "core", [(0, 1), (1, 0)])

    def shift(pair, perm):
        return [lax.ppermute(a, "z", perm) for a in pair]

    mine, send = pack_kv(who, prompt_keys, prompt_values, resp_keys, resp_values)
    block = join_kv(parts, who, mine, swap(send))
    half = HEADS // 2 * D
    away = (1 - core) * half
    q_send = lax.dynamic_slice_in_dim(queries, away, half, axis=2)
    c_send = lax.dynamic_slice_in_dim(cotangent, away, half, axis=2)
    q, u = prep(who, queries, swap(q_send), cotangent, swap(c_send))
    wide = q.shape[1]
    at_rows = z * 2 * rows + jnp.arange(wide, dtype=jnp.int32) % (2 * rows)
    at_rows = jnp.broadcast_to(at_rows, (8, wide))

    def place(step):
        return ((z + step) % ring).astype(jnp.int32)

    far = ring // 2
    held = {0: list(block)}
    for s in range(1, far + 1):
        held[-s] = shift(held[-s + 1], ups)
        if s < far:
            held[s] = shift(held[s - 1], downs)
    st = stats(who, [held[0]], [place(0)], parts, q, u, at_rows, None)
    for s in range(1, far + 1):
        steps = (-s, s) if s < far else (-s,)
        st = stats(
            who, [held[k] for k in steps], [place(k) for k in steps], parts, q, u, at_rows, st
        )

    def added(terms, arrived):
        if arrived is not None:
            terms = [t + a.astype(f32) for t, a in zip(terms, arrived)]
        return [t.astype(bf16) for t in terms]

    dq, own, going_down, going_up = None, None, None, None
    for s in range(far, 0, -1):
        steps = (-s, s) if s < far else (-s, 0)
        terms, dq = grads(
            who, [held[k] for k in steps], [place(k) for k in steps], parts, q, u, at_rows, st, dq
        )
        low = added(terms[0], going_down)
        if s == far:
            own, high = terms[1], None
        else:
            high = added(terms[1], going_up)
        dq, low, high = lax.optimization_barrier((dq, low, high))
        going_down = shift(low, downs)
        if high is not None:
            going_up = shift(high, ups)

    dq_own, dq_other = finish(who, dq, rows)
    dq_rest = swap(dq_other)
    grad_queries = jnp.where(
        core == 0,
        jnp.concatenate([dq_own, dq_rest], axis=2),
        jnp.concatenate([dq_rest, dq_own], axis=2),
    )
    mine, send = split_rows(parts, who, own, [going_down, going_up])
    return (grad_queries, *emit(parts, who, mine, swap(send)))


def solution(mesh):
    ring = mesh.shape["ctx"] // 2
    torus = Mesh(mesh.devices.reshape(mesh.shape["pairs"], ring, 2), ("pairs", "z", "core"))
    both, ctx = P(("pairs", "z", "core"), None), P("pairs", ("z", "core"), None)
    return jax.shard_map(
        local,
        mesh=torus,
        in_specs=(both, both, ctx, ctx, ctx, ctx, P("pairs")),
        out_specs=(ctx, ctx, ctx, both, both),
        check_vma=False,
    )
```

```python
import functools
import math

import jax
import jax.numpy as jnp
from jax import lax
from jax.experimental import pallas as pl
from jax.experimental.pallas import tpu as pltpu
from jax.sharding import Mesh
from jax.sharding import PartitionSpec as P


HEADS = 32
KV_HEADS = 4
D = 128
GROUP = HEADS // KV_HEADS
OWN = KV_HEADS // 2
SCALE = D ** (-0.5)
TO_LOG2 = SCALE * math.log2(math.e)
LOW = -1e30
COLS = 256


f32 = jnp.float32
bf16 = jnp.bfloat16
VMEM = pl.BlockSpec(memory_space=pltpu.VMEM)
SMEM = pl.BlockSpec(memory_space=pltpu.SMEM)
SMALL = pltpu.CompilerParams(vmem_limit_bytes=16 * 2**20)


def nt(a, b):
    return lax.dot_general(a, b, (((1,), (1,)), ((), ())), preferred_element_type=f32)


def nn(a, b):
    return lax.dot_general(a, b, (((1,), (0,)), ((), ())), preferred_element_type=f32)


def cost(flops, nbytes):
    return pl.CostEstimate(flops=int(flops), bytes_accessed=int(nbytes), transcendentals=0)


def pack_kernel(pk, pv, rk, rv, mine, send):
    core = lax.axis_index("core")
    prompt, rows = pk.shape[0], rk.shape[1]
    for dst, side in ((mine, core), (send, 1 - core)):
        for j in range(OWN):
            lanes = pl.ds(pl.multiple_of((side * OWN + j) * D, D), D)
            for k, (p_ref, r_ref) in enumerate(((pk, rk), (pv, rv))):
                out = pl.ds(k * D, D)
                dst[j, 0:prompt, out] = p_ref[:, lanes]
                for b in range(2):
                    at = prompt + b * rows
                    dst[j, at : at + rows, out] = r_ref[b, :, lanes]


def pack_kv(pk, pv, rk, rv):
    rows = pk.shape[0] + 2 * rk.shape[1]
    shape = jax.ShapeDtypeStruct((OWN, rows, 2 * D), bf16)
    return pl.pallas_call(
        pack_kernel,
        out_shape=(shape, shape),
        in_specs=[VMEM] * 4,
        out_specs=(VMEM, VMEM),
        name="pack_kv",
    )(pk, pv, rk, rv)


def parts_of(prompt, rows):
    return (
        (0, 0, prompt),
        (prompt, 2 * prompt, rows),
        (prompt + rows, 2 * prompt + 2 * rows, rows),
    )


def join_kernel(parts, mine, other, out):
    core = lax.axis_index("core")
    tall = out.shape[0] // OWN
    for src, side in ((mine, core), (other, 1 - core)):
        for j in range(OWN):
            for at, chip_at, n in parts:
                to = pl.ds(pl.multiple_of(j * tall + chip_at + side * n, 16), n)
                out[to, :] = src[j, at : at + n, :]


def join_kv(parts, mine, other):
    return pl.pallas_call(
        functools.partial(join_kernel, parts),
        out_shape=jax.ShapeDtypeStruct((OWN * 2 * mine.shape[1], 2 * D), bf16),
        in_specs=[VMEM, VMEM],
        out_specs=VMEM,
        compiler_params=SMALL,
        name="join_kv",
    )(mine, other)


def prep_kernel(who, q_all, c_all, other, q_out, u_out):
    place, core = who[0], who[1]
    rows = q_all.shape[1]

    def step(hb, _):
        h, b = hb // 2, hb % 2
        for side, q_ref, c_ref, base in (
            (core, q_all, c_all, core * OWN + h),
            (1 - core, other.at[0], other.at[1], h),
        ):
            first = place * (2 * rows) + side * rows
            alive = first + lax.broadcasted_iota(jnp.int32, (rows, D), 0) < who[2 + b]
            for g in range(GROUP):
                to = pl.ds(pl.multiple_of(g * 2 * rows + side * rows, 16), rows)
                lanes = pl.ds(pl.multiple_of((base * GROUP + g) * D, D), D)
                q_out[hb, to, :] = q_ref[b, :, lanes]
                u = c_ref[b, :, lanes].astype(f32)
                u_out[hb, to, :] = jnp.where(alive, u, 0.0).astype(bf16)
        return 0

    lax.fori_loop(0, 2 * OWN, step, 0)


def prep(who, q_all, c_all, other):
    rows = q_all.shape[1]
    shape = jax.ShapeDtypeStruct((OWN * 2, 2 * rows * GROUP, D), bf16)
    return pl.pallas_call(
        prep_kernel,
        out_shape=(shape, shape),
        in_specs=[SMEM] + [VMEM] * 3,
        out_specs=(VMEM, VMEM),
        compiler_params=SMALL,
        cost_estimate=cost(1e6, 6e6),
        name="prep",
    )(who, q_all, c_all, other)


def load_keys(blocks, parts, h, b, ks, vs):
    prompt, rows = 2 * parts[0][2], 2 * parts[1][2]
    n = len(blocks)
    tall = blocks[0].shape[0] // OWN
    top = pl.ds(pl.multiple_of(h * tall, 16), prompt)
    low = pl.ds(pl.multiple_of(h * tall + prompt + b * rows, 16), rows)
    for i, ref in enumerate(blocks):
        ks[i * prompt : (i + 1) * prompt, :] = ref[top, :D]
        vs[i * prompt : (i + 1) * prompt, :] = ref[top, D:]
        at = n * prompt + i * rows
        ks[at : at + rows, :] = ref[low, :D]
        vs[at : at + rows, :] = ref[low, D:]


def spans(n, parts):
    prompt, rows = 2 * parts[0][2], 2 * parts[1][2]
    out = [(0, n * prompt, None)]
    return out + [(n * prompt + i * rows, rows, i) for i in range(n)]


def seen_block(who, ring, step):
    return lax.rem(who[0] + (step + ring), ring) < who[0]


def own_mask(rows, cols, t):
    row = lax.rem(lax.broadcasted_iota(jnp.int32, (1, cols), 1) + t * cols, rows)
    return lax.broadcasted_iota(jnp.int32, (rows, cols), 0) <= row


def by_eights(x):
    return x.reshape(x.shape[0] // 8, 8, x.shape[1])


def stats_kernel(steps, ring, parts, first, last, *refs):
    n = len(steps)
    who, blocks, refs = refs[0], refs[1 : 1 + n], refs[1 + n :]
    q_ref, u_ref, refs = refs[0], refs[1], refs[2:]
    if first:
        old, (out, ks, vs) = None, refs
    else:
        old, out, ks, vs = refs
    valid = [seen_block(who, ring, k) for k in steps]

    def head(hb, _):
        load_keys(blocks, parts, hb // 2, hb % 2, ks, vs)
        for t in range(q_ref.shape[1] // COLS):
            cols = slice(t * COLS, (t + 1) * COLS)
            s = nt(ks[...], q_ref[hb, cols, :]) * TO_LOG2
            dp = nt(vs[...], u_ref[hb, cols, :])
            peak = LOW if first else old[hb, 0, :, cols]
            xs = []
            for at, rows, i in spans(n, parts):
                x = s[at : at + rows]
                if i is not None and steps[i] == 0:
                    x = jnp.where(own_mask(rows, COLS, t), x, -jnp.inf)
                top = jnp.max(by_eights(x), axis=0)
                if i is not None and steps[i] != 0:
                    top = jnp.where(valid[i], top, LOW)
                peak = jnp.maximum(peak, top)
                xs.append(x)
            total, dot = 0.0, 0.0
            if not first:
                fade = jnp.exp2(old[hb, 0, :, cols] - peak)
                total, dot = old[hb, 1, :, cols] * fade, old[hb, 2, :, cols] * fade
            for x, (at, rows, i) in zip(xs, spans(n, parts)):
                lift = peak
                if i is not None and steps[i] != 0:
                    lift = jnp.where(valid[i], peak, jnp.inf)
                p = jnp.exp2(by_eights(x) - lift[None])
                total = total + jnp.sum(p, axis=0)
                dot = dot + jnp.sum(p * by_eights(dp[at : at + rows]), axis=0)
            if last:
                best = jnp.max(peak, axis=0, keepdims=True)
                fade = jnp.exp2(peak - best)
                whole = jnp.sum(total * fade, axis=0, keepdims=True)
                delta = jnp.sum(dot * fade, axis=0, keepdims=True) / whole
                out[hb, 0, :, cols] = jnp.broadcast_to(best + jnp.log2(whole), peak.shape)
                out[hb, 1, :, cols] = jnp.broadcast_to(delta, peak.shape)
            else:
                out[hb, 0, :, cols] = peak
                out[hb, 1, :, cols] = total
                out[hb, 2, :, cols] = dot
        return 0

    lax.fori_loop(0, 2 * OWN, head, 0)


def stats(who, steps, ring, blocks, parts, q, u, old, last):
    n = len(blocks)
    wide = q.shape[1]
    keys = n * 2 * (parts[0][2] + parts[1][2])
    operands = [who, *blocks, q, u] + ([] if old is None else [old])
    return pl.pallas_call(
        functools.partial(stats_kernel, steps, ring, parts, old is None, last),
        out_shape=jax.ShapeDtypeStruct((OWN * 2, 2 if last else 3, 8, wide), f32),
        in_specs=[SMEM] + [VMEM] * (len(operands) - 1),
        out_specs=VMEM,
        scratch_shapes=[pltpu.VMEM((keys, D), bf16), pltpu.VMEM((keys, D), bf16)],
        compiler_params=SMALL,
        cost_estimate=cost(4 * 12 * keys * wide * D, 3e6),
    )(*operands)


def grads_kernel(steps, ring, parts, first, *refs):
    n = len(steps)
    who, blocks, refs = refs[0], refs[1 : 1 + n], refs[1 + n :]
    q_ref, u_ref, st, refs = refs[0], refs[1], refs[2], refs[3:]
    if not first:
        dq_in, refs = refs[0], refs[1:]
    terms, (dq, ks, vs, ps, ds) = refs[:n], refs[n:]
    prompt, rows = 2 * parts[0][2], 2 * parts[1][2]
    tall = blocks[0].shape[0] // OWN
    valid = [seen_block(who, ring, k) for k in steps]

    def head(hb, _):
        h, b = hb // 2, hb % 2
        load_keys(blocks, parts, h, b, ks, vs)
        kt = ks[...].T
        for t in range(q_ref.shape[1] // COLS):
            cols = slice(t * COLS, (t + 1) * COLS)
            s = nt(ks[...], q_ref[hb, cols, :]) * TO_LOG2
            dp = nt(vs[...], u_ref[hb, cols, :])
            norm, delta = st[hb, 0, :, cols], st[hb, 1, :, cols]
            for at, count, i in spans(n, parts):
                lift = norm
                if i is not None and steps[i] != 0:
                    lift = jnp.where(valid[i], norm, jnp.inf)
                x = s[at : at + count]
                if i is not None and steps[i] == 0:
                    x = jnp.where(own_mask(count, COLS, t), x, -jnp.inf)
                p = jnp.exp2(by_eights(x) - lift[None])
                d = p * (by_eights(dp[at : at + count]) - delta[None])
                ps[at : at + count, cols] = p.reshape(count, COLS).astype(bf16)
                ds[at : at + count, cols] = d.reshape(count, COLS).astype(bf16)
            more = nn(kt, ds[:, cols])
            dq[hb, :, cols] = more if first else dq_in[hb, :, cols] + more
        dk = nn(ds[...], q_ref[hb]) * SCALE
        dv = nn(ps[...], u_ref[hb])
        top = pl.ds(pl.multiple_of(h * tall, 16), prompt)
        low = pl.ds(pl.multiple_of(h * tall + prompt + b * rows, 16), rows)
        for i in range(n):
            for lanes, g in ((slice(0, D), dk), (slice(D, 2 * D), dv)):
                out = terms[i]
                before = jnp.where(b == 0, 0.0, out[top, lanes])
                out[top, lanes] = before + g[i * prompt : (i + 1) * prompt]
                at = n * prompt + i * rows
                out[low, lanes] = g[at : at + rows]
        return 0

    lax.fori_loop(0, 2 * OWN, head, 0)


def grads(who, steps, ring, blocks, parts, q, u, st, dq):
    n = len(blocks)
    wide = q.shape[1]
    keys = n * 2 * (parts[0][2] + parts[1][2])
    operands = [who, *blocks, q, u, st]
    aliases = {}
    if dq is not None:
        aliases = {len(operands): n}
        operands.append(dq)
    out = pl.pallas_call(
        functools.partial(grads_kernel, steps, ring, parts, dq is None),
        out_shape=(
            *[jax.ShapeDtypeStruct(blocks[0].shape, f32)] * n,
            jax.ShapeDtypeStruct((OWN * 2, D, wide), f32),
        ),
        in_specs=[SMEM] + [VMEM] * (len(operands) - 1),
        out_specs=(VMEM,) * (n + 1),
        scratch_shapes=[
            pltpu.VMEM((keys, D), bf16),
            pltpu.VMEM((keys, D), bf16),
            pltpu.VMEM((keys, wide), bf16),
            pltpu.VMEM((keys, wide), bf16),
        ],
        input_output_aliases=aliases,
        compiler_params=SMALL,
        cost_estimate=cost(4 * 20 * keys * wide * D, 6e6),
    )(*operands)
    return out[:n], out[n]


def add_kernel(pairs, *refs):
    for i in range(pairs):
        term, arrived = refs[2 * i], refs[2 * i + 1]
        refs[2 * pairs + i][...] = (term[...] + arrived[...].astype(f32)).astype(bf16)


def add_all(terms, arrived):
    n = len(terms)
    flat = [a for pair in zip(terms, arrived) for a in pair]
    return pl.pallas_call(
        functools.partial(add_kernel, n),
        out_shape=(jax.ShapeDtypeStruct(terms[0].shape, bf16),) * n,
        in_specs=[VMEM] * len(flat),
        out_specs=(VMEM,) * n,
        compiler_params=SMALL,
    )(*flat)


def finish_kernel(who, dq, own, other, turned):
    core = who[1]
    rows = own.shape[1]

    def step(hb, _):
        h, b = hb // 2, hb % 2
        turned[...] = dq[hb].T * SCALE
        for out, side in ((own, core), (other, 1 - core)):
            for g in range(GROUP):
                at = pl.ds(pl.multiple_of(g * 2 * rows + side * rows, 16), rows)
                lanes = pl.ds(pl.multiple_of((h * GROUP + g) * D, D), D)
                out[b, :, lanes] = turned[at, :]
        return 0

    lax.fori_loop(0, 2 * OWN, step, 0)


def finish(who, dq, rows):
    wide = dq.shape[2]
    shape = jax.ShapeDtypeStruct((2, rows, OWN * GROUP * D), f32)
    return pl.pallas_call(
        finish_kernel,
        out_shape=(shape, shape),
        in_specs=[SMEM, VMEM],
        out_specs=(VMEM, VMEM),
        scratch_shapes=[pltpu.VMEM((wide, D), f32)],
        compiler_params=SMALL,
        cost_estimate=cost(1e6, 4e6),
        name="finish",
    )(who, dq)


def split_kernel(parts, who, *refs):
    ins, (mine, send) = refs[:-2], refs[-2:]
    core = who[1]
    tall = ins[0].shape[0] // OWN
    for dst, side in ((mine, core), (send, 1 - core)):
        for j in range(OWN):
            for at, chip_at, n in parts:
                src = pl.ds(pl.multiple_of(j * tall + chip_at + side * n, 16), n)
                total = ins[0][src, :]
                for more in ins[1:]:
                    total = total + more[src, :].astype(f32)
                dst[j, at : at + n, :] = total


def split_rows(parts, who, own, arrived):
    shape = jax.ShapeDtypeStruct((OWN, own.shape[0] // (2 * OWN), 2 * D), f32)
    return pl.pallas_call(
        functools.partial(split_kernel, parts),
        out_shape=(shape, shape),
        in_specs=[SMEM] + [VMEM] * (1 + len(arrived)),
        out_specs=(VMEM, VMEM),
        compiler_params=SMALL,
        name="split_rows",
    )(who, own, *arrived)


def emit_kernel(parts, who, mine, other, rk, rv, pk, pv):
    core = who[1]
    for src, side in ((mine, core), (other, 1 - core)):
        for j in range(OWN):
            lanes = pl.ds(pl.multiple_of((side * OWN + j) * D, D), D)
            for k, (p_ref, r_ref) in enumerate(((pk, rk), (pv, rv))):
                at, _, n = parts[0]
                p_ref[:, lanes] = src[j, at : at + n, k * D : (k + 1) * D]
                for b in range(2):
                    at, _, n = parts[1 + b]
                    r_ref[b, :, lanes] = src[j, at : at + n, k * D : (k + 1) * D]


def emit(parts, who, mine, other):
    prompt = jax.ShapeDtypeStruct((parts[0][2], KV_HEADS * D), f32)
    resp = jax.ShapeDtypeStruct((2, parts[1][2], KV_HEADS * D), f32)
    return pl.pallas_call(
        functools.partial(emit_kernel, parts),
        out_shape=(resp, resp, prompt, prompt),
        in_specs=[SMEM, VMEM, VMEM],
        out_specs=(VMEM,) * 4,
        compiler_params=SMALL,
        name="emit",
    )(who, mine, other)


def local(prompt_keys, prompt_values, queries, resp_keys, resp_values, cotangent, lengths):
    ring = lax.axis_size("z")
    z, core = lax.axis_index("z"), lax.axis_index("core")
    rows = queries.shape[1]
    parts = parts_of(prompt_keys.shape[0], rows)
    who = jnp.stack([z, core, lengths[0], lengths[1]]).astype(jnp.int32)
    ups = [(i, (i + 1) % ring) for i in range(ring)]
    downs = [(i, (i - 1) % ring) for i in range(ring)]

    def swap(x):
        return lax.ppermute(x, "core", [(0, 1), (1, 0)])

    mine, send = pack_kv(prompt_keys, prompt_values, resp_keys, resp_values)
    block = join_kv(parts, mine, swap(send))
    half = HEADS // 2 * D
    away = (1 - core) * half
    q_send, c_send = (
        lax.dynamic_slice_in_dim(x, away, half, axis=2) for x in (queries, cotangent)
    )
    q, u = prep(who, queries, cotangent, swap(jnp.stack([q_send, c_send])))

    far = ring // 2
    held = {0: block}
    up, down = block, block
    for s in range(1, far + 1):
        up = lax.ppermute(up, "z", ups)
        held[-s] = up
        if s < far:
            down = lax.ppermute(down, "z", downs)
            held[s] = down
            up, down = lax.optimization_barrier((up, down))
            held[-s], held[s] = up, down
    st = stats(who, (0,), ring, [held[0]], parts, q, u, None, False)
    for s in range(1, far + 1):
        steps = (-s, s) if s < far else (-s,)
        st = stats(who, steps, ring, [held[k] for k in steps], parts, q, u, st, s == far)

    def terms_of(steps, dq):
        return grads(who, steps, ring, [held[k] for k in steps], parts, q, u, st, dq)

    dq, down, up = None, None, None
    for s in range(far, 0, -1):
        terms, dq = terms_of((-s, s) if s < far else (-s,), dq)
        if s == far:
            low, high = terms[0].astype(bf16), None
        elif s == far - 1:
            (low,), high = add_all(terms[:1], [down]), terms[1].astype(bf16)
        else:
            low, high = add_all(terms, [down, up])
        dq, low, high = lax.optimization_barrier((dq, low, high))
        down = lax.ppermute(low, "z", downs)
        if high is not None:
            up = lax.ppermute(high, "z", ups)
    (own,), dq = terms_of((0,), dq)

    dq_own, dq_other = finish(who, dq, rows)
    dq_rest = swap(dq_other)
    grad_queries = jnp.where(
        core == 0,
        jnp.concatenate([dq_own, dq_rest], axis=2),
        jnp.concatenate([dq_rest, dq_own], axis=2),
    )
    mine, send = split_rows(parts, who, own, [down, up])
    return (grad_queries, *emit(parts, who, mine, swap(send)))


def solution(mesh):
    ring = mesh.shape["ctx"] // 2
    torus = Mesh(mesh.devices.reshape(mesh.shape["pairs"], ring, 2), ("pairs", "z", "core"))
    both, ctx = P(("pairs", "z", "core"), None), P("pairs", ("z", "core"), None)

    return jax.shard_map(
        local,
        mesh=torus,
        in_specs=(both, both, ctx, ctx, ctx, ctx, P("pairs")),
        out_specs=(ctx, ctx, ctx, both, both),
        check_vma=False,
    )
```
